512 devices in a mesh: dp: 128 (over z, y, core), tensor: 4 (over x).
Axes of the slice: x: 4, y: 8, z: 8, core: 2. Of those that a mesh axis runs over, the one named last changes fastest.
Arguments:
- hidden: bfloat16 [512, 8, 3584], P('dp', None, 'tensor')
- norm_gain: float32 [3584], replicated, may hold values from 0.5 to 2
- head_weight: bfloat16 [152064, 3584], P(('dp', 'tensor'))
- counts: int32 [128], P('dp'), may hold values from 1 to 3, as said below
- destination: int32 [512], P('dp'), may hold values from 0 to 127, as said below
- lengths: int32 [512], P('dp'), may hold values from 1 to 8
- labels: int32 [512, 8], P('dp'), may hold values from 0 to 152063
Outputs:
- scores: float32 [256], P('dp')
The draws below stay inside these ranges and needn't reach their ends.
Inputs may be any that keep to these rules, and one draw needn't show every extreme that they name: The first counts[i] slots of index i are live; the counts sum to 256. The live slots of index i go to i or to i + 1, lower slots first to i; every index of dp is the destination of exactly 2 live slots; at most 1 live slots of one index go to the next index, a bound reached in every draw; entries of slots that are not live are arbitrary.
All inputs are finite; a program needn't handle non-finite values.
Results may differ from the reference program's by a relative error of at most 0.0025.
Values may be sent and summed in bfloat16 or wider, within the bound.
No kernel may reach another device: no remote copies, remote signals or barrier semaphores. Data moves between devices by JAX's collectives and lax.ppermute only.
A program may use at most 64 MiB of HBM per device.

```python
import math
import jax
import jax.numpy as jnp
from jax import lax

D = 3584
VOCAB = 152064
BLOCK = 8
BLK_DEV = 2
CAP = 4
SLOTS = 512
TOKENS = 2048
N_DP = 128


def label_table(key):
    return jax.random.randint(jax.random.fold_in(key, 31), (SLOTS, BLOCK), 0, VOCAB).astype(jnp.int32)


def vocab_row(key, index):
    return jax.random.normal(jax.random.fold_in(jax.random.fold_in(key, 47), index), (D,), jnp.float32)


def draw_head_weight(key, part):
    rows = jax.vmap(lambda index: vocab_row(key, index))(jnp.arange(VOCAB, dtype=jnp.int32))
    return (rows * (5.5 / math.sqrt(D))).astype(jnp.bfloat16)


def draw_labels(key, part):
    return label_table(key)


def draw_hidden(key, part):
    targets = label_table(key).reshape(-1)
    total = targets.shape[0]
    aligned = jax.vmap(lambda index: vocab_row(key, index))(targets)
    noise = jax.random.normal(jax.random.fold_in(key, 53), (total, D), jnp.float32)
    strength = jax.random.uniform(jax.random.fold_in(key, 59), (total, 1), jnp.float32, 0.0, 0.12)
    rows = noise + strength * aligned
    return rows.reshape(SLOTS, BLOCK, D).astype(jnp.bfloat16)


def block_layout(key):
    devices = SLOTS // CAP
    inner = jax.random.randint(jax.random.fold_in(key, 79), (devices - 1,), 0, BLK_DEV).astype(jnp.int32)
    forced = jax.random.randint(jax.random.fold_in(key, 83), (), 0, devices - 1).astype(jnp.int32)
    inner = inner.at[forced].set(BLK_DEV - 1)
    inner = inner.at[0].set(BLK_DEV - 1)
    zero_end = jnp.zeros((1,), jnp.int32)
    excess = jnp.concatenate([zero_end, inner, zero_end])
    counts = (BLK_DEV + excess[1:] - excess[:-1]).astype(jnp.int32)
    device_ids = jnp.arange(devices, dtype=jnp.int32)
    start = device_ids * BLK_DEV + excess[:-1]
    slot_ids = jnp.arange(CAP, dtype=jnp.int32)
    global_rank = start[:, None] + slot_ids[None, :]
    live_target = jnp.clip(global_rank // BLK_DEV, 0, devices - 1).astype(jnp.int32)
    filler = jax.random.randint(jax.random.fold_in(key, 97), (devices, CAP), 0, devices).astype(jnp.int32)
    destination = jnp.where(slot_ids[None, :] < counts[:, None], live_target, filler)
    return (counts.astype(jnp.int32), destination.reshape(-1).astype(jnp.int32))


def draw_counts(key, part):
    return block_layout(key)[0]


def draw_destination(key, part):
    return block_layout(key)[1]


def with_ends(entries, rng, low, largest):
    longest = entries.shape.index(max(entries.shape))
    spots = []
    for shift in (0, 1):
        where = [jax.random.randint(jax.random.fold_in(rng, axis), (), 0, length) for axis, length in enumerate(entries.shape)]
        where[longest] = (where[longest] + shift) % entries.shape[longest]
        spots.append(tuple(where))
    return entries.at[spots[0]].set(low).at[spots[1]].set(largest)


def setup_inputs(seed: int = 0) -> dict:
    key_list = jax.random.split(jax.random.key(seed), 8)
    hidden = draw_hidden(jax.random.fold_in(key_list[7], 71), 0)
    norm_gain = jnp.clip(jnp.exp(jax.random.uniform(key_list[1], (D,), jnp.float32, math.log(0.5), math.log(2.0))), 0.5, 2.0)
    head_weight = draw_head_weight(jax.random.fold_in(key_list[7], 71), 0)
    counts = draw_counts(jax.random.fold_in(key_list[7], 71), 0)
    destination = draw_destination(jax.random.fold_in(key_list[7], 71), 0)
    lengths = with_ends(jax.random.randint(key_list[5], (SLOTS,), 1, BLOCK + 1), jax.random.fold_in(key_list[5], 1), 1, BLOCK).astype(jnp.int32)
    labels = draw_labels(jax.random.fold_in(key_list[7], 71), 0)
    return {"hidden": hidden, "norm_gain": norm_gain, "head_weight": head_weight, "counts": counts, "destination": destination, "lengths": lengths, "labels": labels}


epsilon = 1e-06

def reference(hidden, norm_gain, head_weight, counts, destination, lengths, labels):
    slot_ids = jnp.arange(SLOTS, dtype=jnp.int32)
    source = slot_ids // CAP
    is_live = slot_ids % CAP < counts[source]
    sort_key = jnp.where(is_live, destination, N_DP).astype(jnp.int32)
    order = jnp.argsort(sort_key, stable=True)[:N_DP * BLK_DEV]
    rows = hidden[order].reshape(TOKENS, D).astype(jnp.float32)
    row_labels = labels[order].reshape(TOKENS)
    block_lengths = lengths[order]
    mean_square = lax.optimization_barrier(jnp.mean(rows * rows, axis=-1, keepdims=True))
    normed = (rows * lax.rsqrt(mean_square + epsilon) * norm_gain).astype(jnp.bfloat16)
    groups = N_DP // 8

    def score_group(inputs):
        group_rows, group_labels = inputs
        logits = lax.dot_general(group_rows, head_weight, (((1,), (1,)), ((), ())), preferred_element_type=jnp.float32)
        row_peak = lax.optimization_barrier(jnp.max(logits, axis=1))
        scaled = jnp.exp(logits - row_peak[:, None])
        exp_sum = lax.optimization_barrier(jnp.sum(scaled, axis=1))
        square_sum = lax.optimization_barrier(jnp.sum(scaled * scaled, axis=1))
        label_logit = jnp.take_along_axis(logits, group_labels[:, None], axis=1)[:, 0]
        return square_sum / (exp_sum * exp_sum) - 2.0 * jnp.exp(label_logit - row_peak) / exp_sum + 1.0
    token_error = lax.map(score_group, (normed.reshape(groups, -1, D), row_labels.reshape(groups, -1)))
    token_error = token_error.reshape(N_DP * BLK_DEV, BLOCK)
    valid = jnp.arange(BLOCK, dtype=jnp.int32)[None, :] < block_lengths[:, None]
    return lax.optimization_barrier(jnp.sum(jnp.where(valid, token_error, jnp.float32(0.0)), axis=1)) / block_lengths.astype(jnp.float32)
```

```python
import jax
import jax.numpy as jnp
from jax import lax
from jax.sharding import Mesh
from jax.sharding import PartitionSpec as P

BLK_DEV = 2
DP = ("dp_0", "dp_1", "dp_2")
DP_TENSOR = ("dp_0", "dp_1", "dp_2", "tensor")

GRID = (8, 8)
epsilon = 1e-06


def from_behind(block):
    devices = lax.axis_size(DP)
    return lax.ppermute(block, DP, [(i, i + 1) for i in range(devices - 1)])


def to_everyone(shard, axes):
    copies = jnp.broadcast_to(shard[None], (lax.axis_size(axes), *shard.shape))
    return lax.all_to_all(copies, axes, split_axis=0, concat_axis=0, tiled=True)


def received(stay, arrived, own):
    from_last = stay < BLK_DEV
    return jnp.where(
        from_last, jnp.stack([arrived, own[0]]), jnp.stack([own[0], own[1]])
    )


def normalize(rows, norm_gain):
    values = rows.astype(jnp.float32)
    mean_square = jnp.mean(values * values, axis=-1, keepdims=True)
    return (values * lax.rsqrt(mean_square + epsilon) * norm_gain).astype(jnp.bfloat16)


def per_device(hidden, norm_gain, head_weight, counts, destination, lengths, labels):
    capacity, block_len, quarter_width = hidden.shape
    dp_size = lax.axis_size(DP)
    tensor_ways = lax.axis_size("tensor")
    dp_index = lax.axis_index(DP)
    tensor_index = lax.axis_index("tensor")
    tokens = BLK_DEV * block_len
    is_live = jnp.arange(capacity, dtype=jnp.int32) < counts[0]
    stay = jnp.sum(is_live & (destination == dp_index)).astype(jnp.int32)
    stay = jnp.clip(stay, 1, BLK_DEV)
    leaving = jnp.where(stay == 1, hidden[1], hidden[2])
    facts = jnp.concatenate([labels, lengths[:, None]], axis=1)
    leaving_facts = jnp.where(stay == 1, facts[1], facts[2])
    arrived = from_behind(leaving)
    arrived_facts = from_behind(leaving_facts)
    local = received(stay, arrived, hidden).reshape(tokens, quarter_width)
    gathered = to_everyone(local, "tensor")
    gathered = jnp.moveaxis(gathered, 0, 1).reshape(tokens, tensor_ways * quarter_width)
    normed = normalize(gathered, norm_gain)
    local_facts = received(stay, arrived_facts, facts)
    local_labels = local_facts[:, :block_len].reshape(tokens)
    local_lengths = local_facts[:, block_len]

    rows = lax.all_gather(normed, DP, axis=0, tiled=True)
    row_labels = lax.all_gather(local_labels, DP, axis=0, tiled=True)
    vocab_rows = head_weight.shape[0]
    vocab_start = (dp_index * tensor_ways + tensor_index) * vocab_rows
    logits = lax.dot_general(
        rows, head_weight, (((1,), (1,)), ((), ())), preferred_element_type=jnp.float32
    )
    row_peak = jnp.max(logits, axis=1)
    scaled = jnp.exp(logits - row_peak[:, None])
    vocab_ids = vocab_start + jnp.arange(vocab_rows, dtype=jnp.int32)
    hit = vocab_ids[None, :] == row_labels[:, None]
    stats = jnp.stack(
        [
            row_peak.reshape(dp_size, tokens),
            jnp.sum(scaled, axis=1).reshape(dp_size, tokens),
            jnp.sum(scaled * scaled, axis=1).reshape(dp_size, tokens),
            jnp.sum(jnp.where(hit, logits, 0.0), axis=1).reshape(dp_size, tokens),
        ],
        axis=1,
    ).reshape(dp_size, 1, 4 * tokens)
    outgoing = jnp.broadcast_to(stats, (dp_size, tensor_ways, 4 * tokens))
    parts = lax.all_to_all(
        outgoing.reshape(dp_size * tensor_ways, 4 * tokens),
        DP_TENSOR,
        split_axis=0,
        concat_axis=0,
        tiled=True,
    )
    part_peak = parts[:, :tokens]
    peak = jnp.max(part_peak, axis=0)
    rescale = jnp.exp(part_peak - peak[None, :])
    exp_sum = jnp.sum(parts[:, tokens : 2 * tokens] * rescale, axis=0)
    square_sum = jnp.sum(parts[:, 2 * tokens : 3 * tokens] * rescale * rescale, axis=0)
    label_logit = jnp.sum(parts[:, 3 * tokens :], axis=0)
    token_error = (
        square_sum / (exp_sum * exp_sum) - 2.0 * jnp.exp(label_logit - peak) / exp_sum + 1.0
    ).reshape(BLK_DEV, block_len)
    valid = jnp.arange(block_len, dtype=jnp.int32)[None, :] < local_lengths[:, None]
    return jnp.sum(jnp.where(valid, token_error, 0.0), axis=1) / local_lengths.astype(jnp.float32)


def solution(mesh):
    dp, tensor = mesh.shape["dp"], mesh.shape["tensor"]
    finer = Mesh(mesh.devices.reshape(*GRID, dp // (GRID[0] * GRID[1]), tensor), DP_TENSOR)
    placed = (P(DP, None, "tensor"), P(), P(DP_TENSOR, None), P(DP), P(DP), P(DP), P(DP, None))
    return jax.shard_map(per_device, mesh=finer, in_specs=placed, out_specs=P(DP), check_vma=False)
```

```python
import functools

import jax
import jax.numpy as jnp
from jax import lax
from jax.experimental import pallas as pl
from jax.experimental.pallas import tpu as pltpu
from jax.sharding import Mesh
from jax.sharding import PartitionSpec as P


BLK_DEV = 2
DP = ("dp_0", "dp_1", "dp_2")
PLANE = ("dp_0", "dp_1")
SPACE = ("dp_0", "dp_1", "tensor")
DP_TENSOR = ("dp_0", "dp_1", "dp_2", "tensor")

GRID = (8, 8)
INTERPRET = False
epsilon = 1e-06
NOTES = 128
STATS = 4


def around(block, axis, step):
    size = lax.axis_size(axis)
    return lax.ppermute(block, axis, [(i, (i + step) % size) for i in range(size)])


def from_behind(block):
    devices = lax.axis_size(DP)
    return lax.ppermute(block, DP, [(i, i + 1) for i in range(devices - 1)])


def exchange(pieces, axes):
    return lax.all_to_all(pieces, axes, split_axis=0, concat_axis=0, tiled=True)


def to_everyone(shard, axes):
    return exchange(jnp.broadcast_to(shard[None], (lax.axis_size(axes), *shard.shape)), axes)


def arrange_body(per_source, received, tokens, notes):
    ways, _, width = tokens.shape
    group = min(256, received.shape[0])
    share = group // ways
    row = lax.broadcasted_iota(jnp.int32, (group, group), 0)
    column = lax.broadcasted_iota(jnp.int32, (group, group), 1)
    token = row % share
    wanted = token // per_source * (ways * per_source) + token % per_source
    wanted = wanted + row // share * per_source
    pick = jnp.where(column == wanted, 1.0, 0.0).astype(jnp.bfloat16)
    for block in range(received.shape[0] // group):
        rows = received[block * group : (block + 1) * group, :]
        placed = jnp.dot(pick, rows, preferred_element_type=jnp.float32).astype(jnp.bfloat16)
        here = slice(block * share, (block + 1) * share)
        for q in range(ways):
            tokens[q, here, :] = placed[q * share : (q + 1) * share, :width]
        notes[here, :] = placed[:share, width:]


def arranged(received, ways, per_source, width):
    vmem = pl.BlockSpec(memory_space=pltpu.VMEM)
    count = received.shape[0] // ways
    return pl.pallas_call(
        functools.partial(arrange_body, per_source),
        out_shape=(
            jax.ShapeDtypeStruct((ways, count, width), jnp.bfloat16),
            jax.ShapeDtypeStruct((count, NOTES), jnp.bfloat16),
        ),
        in_specs=[vmem],
        out_specs=(vmem, vmem),
        interpret=INTERPRET,
        compiler_params=pltpu.CompilerParams(vmem_limit_bytes=16 * 1024 * 1024),
    )(received)


def absorb_body(layout, vocab_rows, starts, tokens, notes, carried, *refs):
    pieces = sum(len(rows) for rows in layout)
    sources, stats, held, arrival = refs[:pieces], refs[pieces], refs[pieces + 1 : -1], refs[-1]
    copies = []
    for chunk, rows in enumerate(layout):
        at = 0
        for size in rows:
            index = len(copies)
            target = held[chunk] if len(rows) == 1 else held[chunk].at[pl.ds(at, size)]
            copies.append(pltpu.make_async_copy(sources[index], target, arrival.at[index]))
            at += size
    for copy in copies:
        copy.start()
    quarters, _, width = tokens.shape
    lane = lax.broadcasted_iota(jnp.int32, (8, NOTES), 1)
    powers = jnp.where(lane == 0, 1.0, jnp.where(lane == 1, 256.0, 65536.0))
    powers = jnp.where(lane < 3, powers, 0.0).astype(jnp.bfloat16)
    labels = lax.dot_general(
        powers, notes[...], (((1,), (1,)), ((), ())), preferred_element_type=jnp.float32
    )[0:1].astype(jnp.int32)
    peak, exp_sum, square_sum, label_logit = (carried[i : i + 1, :] for i in range(STATS))
    waiting = iter(copies)
    for chunk, rows in enumerate(layout):
        for _ in rows:
            next(waiting).wait()
        logits = sum(
            lax.dot_general(
                held[chunk][:, q * width : (q + 1) * width],
                tokens[q],
                (((1,), (1,)), ((), ())),
                preferred_element_type=jnp.float32,
            )
            for q in range(quarters)
        )
        ids = lax.broadcasted_iota(jnp.int32, logits.shape, 0)
        if sum(rows) > vocab_rows:
            logits = jnp.where(ids < vocab_rows, logits, -jnp.inf)
        new_peak = jnp.maximum(peak, jnp.max(logits, axis=0, keepdims=True))
        rescale = jnp.exp(peak - new_peak)
        scaled = jnp.exp(logits - new_peak)
        hit = ids == labels - starts[chunk]
        exp_sum = exp_sum * rescale + jnp.sum(scaled, axis=0, keepdims=True)
        square_sum = square_sum * (rescale * rescale) + jnp.sum(
            scaled * scaled, axis=0, keepdims=True
        )
        label_logit = label_logit + jnp.sum(jnp.where(hit & (ids < vocab_rows), logits, 0.0), axis=0, keepdims=True)
        peak = new_peak
    stats[0:1, :] = peak
    stats[1:2, :] = exp_sum
    stats[2:3, :] = square_sum
    stats[3:4, :] = label_logit
    stats[4:8, :] = jnp.zeros((4, stats.shape[1]), jnp.float32)


def absorbed(carried, tokens, notes, chunks, vocab_rows):
    starts = jnp.stack([start for start, _ in chunks])
    pieces = [piece for _, held in chunks for piece in held]
    layout = [[piece.shape[0] for piece in held] for _, held in chunks]
    depth = pieces[0].shape[1]
    rows = sum(piece.shape[0] for piece in pieces)
    vmem = pl.BlockSpec(memory_space=pltpu.VMEM)
    return pl.pallas_call(
        functools.partial(absorb_body, layout, vocab_rows),
        out_shape=jax.ShapeDtypeStruct(carried.shape, jnp.float32),
        in_specs=[pl.BlockSpec(memory_space=pltpu.SMEM), vmem, vmem, vmem]
        + [pl.BlockSpec(memory_space=pl.ANY)] * len(pieces),
        out_specs=vmem,
        scratch_shapes=[pltpu.VMEM((sum(rows), depth), jnp.bfloat16) for rows in layout]
        + [pltpu.SemaphoreType.DMA((len(pieces),))],
        interpret=INTERPRET,
        cost_estimate=pl.CostEstimate(
            flops=2 * rows * tokens.size,
            bytes_accessed=2 * rows * depth,
            transcendentals=rows * tokens.shape[1],
        ),
        compiler_params=pltpu.CompilerParams(vmem_limit_bytes=32 * 1024 * 1024),
    )(starts, tokens, notes, carried, *pieces)


def per_device(hidden, norm_gain, head_weight, counts, destination, lengths, labels):
    capacity, block_len, width = hidden.shape
    ways = lax.axis_size("tensor")
    plane = lax.axis_size(PLANE)
    dp_index = lax.axis_index(DP)
    core_index = lax.axis_index("dp_2")
    tensor_index = lax.axis_index("tensor")
    share = BLK_DEV * block_len // ways
    cuts = block_len // share

    is_live = jnp.arange(capacity, dtype=jnp.int32) < counts[0]
    stay = jnp.sum(is_live & (destination == dp_index)).astype(jnp.int32)
    short = stay < BLK_DEV

    def placed(slots):
        own = jnp.stack([slots[0], jnp.where(short, slots[0], slots[1])])
        leaving = jnp.where(short, slots[1], slots[2])
        return own, leaving

    own, leaving = placed(hidden)
    own = own.reshape(ways, share, width)
    leaving = jnp.tile(leaving.reshape(cuts, share, width), (ways // cuts, 1, 1))
    gathered = exchange(jnp.concatenate([own, leaving], axis=1), "tensor")

    facts = jnp.stack(
        [labels % 256, labels // 256 % 256, labels // 65536]
        + [jnp.broadcast_to(lengths[:, None], labels.shape)],
        axis=-1,
    )
    own_facts, leaving_facts = placed(facts)
    own_lengths = own_facts[:, 0, 3]
    own_facts = lax.dynamic_index_in_dim(
        own_facts.reshape(ways, share, 4), tensor_index, keepdims=False
    )
    leaving_facts = lax.dynamic_index_in_dim(
        leaving_facts.reshape(cuts, share, 4), tensor_index % cuts, keepdims=False
    )
    notes = jnp.concatenate([own_facts, leaving_facts], axis=0).astype(jnp.bfloat16)

    vocab_rows = head_weight.shape[0]
    half = vocab_rows // 2 // 16 * 16
    top, bottom = head_weight[:half], jnp.pad(head_weight[half:], ((0, -vocab_rows % 16), (0, 0)))
    top, bottom, gathered = lax.optimization_barrier((top, bottom, gathered))
    low_top = around(top, "tensor", 1)
    high_bottom = around(bottom, "tensor", -1)

    values = gathered.astype(jnp.float32)
    mean_square = jnp.sum(values * values, axis=(0, 2), keepdims=True) / (ways * width)
    gain = norm_gain.reshape(ways, 1, width)
    normed = (values * lax.rsqrt(mean_square + epsilon) * gain).astype(jnp.bfloat16)
    notes = jnp.pad(notes[None], ((0, ways - 1), (0, 0), (0, NOTES - 4)))
    rows = jnp.concatenate([normed, notes], axis=2)
    arrived = from_behind(rows[:, share:])
    first = tensor_index < cuts
    message = jnp.where(short & first, arrived, rows[:, :share])
    arrived_length = arrived[0, 0, width + 3].astype(jnp.int32)
    local_lengths = jnp.stack([jnp.where(short, arrived_length, own_lengths[0]), own_lengths[1]])

    received = to_everyone(message.reshape(ways * share, width + NOTES), PLANE)
    low_bottom = around(bottom, "tensor", 1)
    high_top = around(top, "tensor", -1)
    far_top = around(low_top, "tensor", 1)
    far_bottom = around(high_bottom, "tensor", -1)

    partner = 1 - core_index
    chip = (lax.axis_index("dp_0") * lax.axis_size("dp_1") + lax.axis_index("dp_1")) * 2

    def start_of(core, step):
        return ((chip + core) * ways + (tensor_index + step) % ways) * vocab_rows

    held = ((0, (head_weight,)), (-1, (low_top, low_bottom)), (1, (high_top, high_bottom)))
    far = (far_top, far_bottom)
    near = [(start_of(core_index, step), pieces) for step, pieces in held]
    near += [
        (start_of(partner, step), [around(piece, "dp_2", 1) for piece in pieces])
        for step, pieces in held
    ]
    own_far = [(start_of(core_index, 2), far)]
    other_far = [(start_of(partner, 2), [around(piece, "dp_2", 1) for piece in far])]

    received = received.reshape(plane * ways * share, width + NOTES)
    tokens, token_notes = arranged(received, ways, share, width)
    empty = jnp.concatenate(
        [
            jnp.full((1, plane * share), -jnp.inf, jnp.float32),
            jnp.zeros((7, plane * share), jnp.float32),
        ]
    )
    stats = absorbed(empty, tokens, token_notes, near, vocab_rows)
    stats = absorbed(stats, tokens, token_notes, own_far, vocab_rows)
    stats = absorbed(stats, tokens, token_notes, other_far, vocab_rows)

    stats = jnp.moveaxis(stats[:STATS].reshape(STATS, plane, share), 1, 0)
    outgoing = jnp.broadcast_to(
        stats.reshape(plane, 1, STATS * share), (plane, ways, STATS * share)
    )
    sums = exchange(outgoing.reshape(plane * ways, STATS * share), SPACE)
    sums = sums.reshape(plane, ways, STATS * share)
    part_peak = sums[..., :share]
    peak = jnp.max(part_peak, axis=0)
    rescale = jnp.exp(part_peak - peak[None])
    exp_sum = jnp.sum(sums[..., share : 2 * share] * rescale, axis=0)
    square_sum = jnp.sum(sums[..., 2 * share : 3 * share] * rescale * rescale, axis=0)
    label_logit = jnp.sum(sums[..., 3 * share :], axis=0)
    token_error = (
        square_sum / (exp_sum * exp_sum) - 2.0 * jnp.exp(label_logit - peak) / exp_sum + 1.0
    ).reshape(BLK_DEV, block_len)
    valid = jnp.arange(block_len, dtype=jnp.int32)[None, :] < local_lengths[:, None]
    return jnp.sum(jnp.where(valid, token_error, 0.0), axis=1) / local_lengths.astype(jnp.float32)


def solution(mesh):
    dp, tensor = mesh.shape["dp"], mesh.shape["tensor"]
    finer = Mesh(mesh.devices.reshape(*GRID, dp // (GRID[0] * GRID[1]), tensor), DP_TENSOR)
    placed = (P(DP, None, "tensor"), P(), P(DP_TENSOR, None), P(DP), P(DP), P(DP), P(DP, None))
    return jax.shard_map(per_device, mesh=finer, in_specs=placed, out_specs=P(DP), check_vma=False)
```

```python
import functools

import jax
import jax.numpy as jnp
from jax import lax
from jax.experimental import pallas as pl
from jax.experimental.pallas import tpu as pltpu
from jax.sharding import Mesh
from jax.sharding import PartitionSpec as P


BLK_DEV = 2
DP = ("dp_0", "dp_1", "dp_2")
PLANE = ("dp_0", "dp_1")
DP_TENSOR = ("dp_0", "dp_1", "dp_2", "tensor")

GRID = (8, 8)
INTERPRET = False
epsilon = 1e-06
NOTES = 128
STATS = 4
VMEM_LIMIT = 32 * 1024 * 1024
AHEAD = 2


def around(block, axis, step):
    size = lax.axis_size(axis)
    return lax.ppermute(block, axis, [(i, (i + step) % size) for i in range(size)])


def from_behind(block):
    devices = lax.axis_size(DP)
    return lax.ppermute(block, DP, [(i, i + 1) for i in range(devices - 1)])


def exchange(pieces, axes):
    return lax.all_to_all(pieces, axes, split_axis=0, concat_axis=0, tiled=True)


def to_everyone(shard, axes):
    return exchange(jnp.broadcast_to(shard[None], (lax.axis_size(axes), *shard.shape)), axes)


def arrange(received, tokens, notes, per_source):
    ways, _, width = tokens.shape
    group = min(256, received.shape[0])
    share = group // ways
    row = lax.broadcasted_iota(jnp.int32, (group, group), 0)
    column = lax.broadcasted_iota(jnp.int32, (group, group), 1)
    token = row % share
    wanted = token // per_source * (ways * per_source) + token % per_source
    wanted = wanted + row // share * per_source
    pick = jnp.where(column == wanted, 1.0, 0.0).astype(jnp.bfloat16)
    for block in range(received.shape[0] // group):
        rows = received[block * group : (block + 1) * group, :]
        placed = jnp.dot(pick, rows, preferred_element_type=jnp.float32).astype(jnp.bfloat16)
        here = slice(block * share, (block + 1) * share)
        for q in range(ways):
            tokens[q, here, :] = placed[q * share : (q + 1) * share, :width]
        notes[here, :] = placed[:share, width:]


def absorb(copies, held, starts, tokens, notes, carried, stats):
    quarters, _, width = tokens.shape
    lane = lax.broadcasted_iota(jnp.int32, (8, NOTES), 1)
    powers = jnp.where(lane == 0, 1.0, jnp.where(lane == 1, 256.0, 65536.0))
    powers = jnp.where(lane < 3, powers, 0.0).astype(jnp.bfloat16)
    labels = lax.dot_general(
        powers, notes[...], (((1,), (1,)), ((), ())), preferred_element_type=jnp.float32
    )[0:1].astype(jnp.int32)
    peak, exp_sum, square_sum, label_logit = (carried[i : i + 1, :] for i in range(STATS))
    for index, chunk in enumerate(held):
        copies[index].wait()
        if index + AHEAD < len(copies):
            copies[index + AHEAD].start()
        logits = sum(
            lax.dot_general(
                chunk[:, q * width : (q + 1) * width],
                tokens[q],
                (((1,), (1,)), ((), ())),
                preferred_element_type=jnp.float32,
            )
            for q in range(quarters)
        )
        ids = lax.broadcasted_iota(jnp.int32, logits.shape, 0)
        new_peak = jnp.maximum(peak, jnp.max(logits, axis=0, keepdims=True))
        rescale = jnp.exp(peak - new_peak)
        scaled = jnp.exp(logits - new_peak)
        hit = ids == labels - starts[index]
        exp_sum = exp_sum * rescale + jnp.sum(scaled, axis=0, keepdims=True)
        square_sum = square_sum * (rescale * rescale) + jnp.sum(
            scaled * scaled, axis=0, keepdims=True
        )
        label_logit = label_logit + jnp.sum(jnp.where(hit, logits, 0.0), axis=0, keepdims=True)
        peak = new_peak
    stats[0:1, :] = peak
    stats[1:2, :] = exp_sum
    stats[2:3, :] = square_sum
    stats[3:4, :] = label_logit
    stats[4:8, :] = jnp.zeros((4, stats.shape[1]), jnp.float32)


def copies_of(sources, held, arrival):
    copies = [
        pltpu.make_async_copy(source, target, arrival.at[index])
        for index, (source, target) in enumerate(zip(sources, held))
    ]
    for copy in copies[:AHEAD]:
        copy.start()
    return copies


def first_body(count, per_source, starts, received, carried, *refs):
    sources, (stats, tokens, notes) = refs[:count], refs[count : count + 3]
    held, arrival = refs[count + 3 : -1], refs[-1]
    copies = copies_of(sources, held, arrival)
    arrange(received, tokens, notes, per_source)
    absorb(copies, held, starts, tokens, notes, carried, stats)


def next_body(count, starts, tokens, notes, carried, *refs):
    sources, stats, held, arrival = refs[:count], refs[count], refs[count + 1 : -1], refs[-1]
    copies = copies_of(sources, held, arrival)
    absorb(copies, held, starts, tokens, notes, carried, stats)


def absorbed(body, inputs, chunks, count, outputs):
    starts = jnp.stack([start for _, start in chunks])
    arrays = [chunk for chunk, _ in chunks]
    rows, depth = sum(chunk.shape[0] for chunk in arrays), arrays[0].shape[1]
    vmem = pl.BlockSpec(memory_space=pltpu.VMEM)
    return pl.pallas_call(
        body,
        out_shape=outputs,
        in_specs=[pl.BlockSpec(memory_space=pltpu.SMEM)]
        + [vmem] * len(inputs)
        + [pl.BlockSpec(memory_space=pl.ANY if INTERPRET else pltpu.HBM)] * len(arrays),
        out_specs=[vmem] * len(outputs),
        scratch_shapes=[pltpu.VMEM(chunk.shape, chunk.dtype) for chunk in arrays]
        + [pltpu.SemaphoreType.DMA((len(arrays),))],
        interpret=INTERPRET,
        cost_estimate=pl.CostEstimate(
            flops=2 * rows * count * depth,
            bytes_accessed=2 * rows * depth,
            transcendentals=rows * count,
        ),
        compiler_params=pltpu.CompilerParams(vmem_limit_bytes=VMEM_LIMIT),
    )(starts, *inputs, *arrays)


def per_device(hidden, norm_gain, head_weight, counts, destination, lengths, labels):
    capacity, block_len, width = hidden.shape
    ways = lax.axis_size("tensor")
    tall, wide = lax.axis_size("dp_0"), lax.axis_size("dp_1")
    plane = tall * wide
    dp_index = lax.axis_index(DP)
    core_index = lax.axis_index("dp_2")
    tensor_index = lax.axis_index("tensor")
    share = BLK_DEV * block_len // ways
    cuts = block_len // share
    row_width = width + NOTES

    sliced = jnp.moveaxis(hidden.reshape(capacity, cuts, share, width), 1, 0)
    sliced = sliced.reshape(cuts, capacity * share, width)
    gathered = exchange(jnp.tile(sliced, (ways // cuts, 1, 1)), "tensor")

    vocab_rows = head_weight.shape[0]
    half = vocab_rows // 2 // 16 * 16
    weight, gathered, counts, destination, labels, lengths = lax.optimization_barrier(
        (head_weight, gathered, counts, destination, labels, lengths)
    )
    low = around(weight, "tensor", 1)
    high = around(weight, "tensor", -1)

    values = gathered.astype(jnp.float32)
    mean_square = jnp.sum(values * values, axis=(0, 2), keepdims=True) / (ways * width)
    gain = norm_gain.reshape(ways, 1, width)
    normed = (values * lax.rsqrt(mean_square + epsilon) * gain).astype(jnp.bfloat16)
    normed = normed.reshape(ways, capacity, share, width)

    is_live = jnp.arange(capacity, dtype=jnp.int32) < counts[0]
    stay = jnp.sum(is_live & (destination == dp_index)).astype(jnp.int32)
    short = stay < BLK_DEV
    first = tensor_index < cuts
    from_first = first | short

    facts = jnp.stack(
        [labels % 256, labels // 256 % 256, labels // 65536]
        + [jnp.broadcast_to(lengths[:, None], labels.shape)],
        axis=-1,
    ).astype(jnp.float32)
    facts = facts.reshape(capacity, cuts, share, 4)
    facts = jnp.where(tensor_index % cuts == 0, facts[:, 0], facts[:, 1]).astype(jnp.bfloat16)

    def with_facts(near_slot, far_slot, nearer):
        rows = jnp.where(nearer, normed[:, near_slot], normed[:, far_slot])
        notes = jnp.where(nearer, facts[near_slot], facts[far_slot])
        notes = jnp.pad(notes[None], ((0, ways - 1), (0, 0), (0, NOTES - 4)))
        return jnp.concatenate([rows, notes], axis=2)

    own = with_facts(0, 1, from_first)
    arrived = from_behind(with_facts(1, 2, short))
    message = jnp.where(short & first, arrived, own)
    arrived_length = arrived[0, 0, width + 3].astype(jnp.int32)
    local_lengths = jnp.where(
        short, jnp.stack([arrived_length, lengths[0]]), jnp.stack([lengths[0], lengths[1]])
    )

    received = to_everyone(message.reshape(ways * share, row_width), PLANE)
    far_low = around(low[:half], "tensor", 1)
    far_high = around(high[half:], "tensor", -1)

    partner = 1 - core_index
    chip = (lax.axis_index("dp_0") * wide + lax.axis_index("dp_1")) * 2

    def start_of(core, step, row=0):
        return ((chip + core) * ways + (tensor_index + step) % ways) * vocab_rows + row

    held = ((weight, 0, 0), (low, -1, 0), (high, 1, 0))
    far = ((far_low, 2, 0), (far_high, 2, half))

    def chunks_of(core, pieces):
        return [(piece, start_of(core, step, row)) for piece, step, row in pieces]

    def crossed(pieces):
        return [(around(piece, "dp_2", 1), step, row) for piece, step, row in pieces]

    count = plane * share
    received = received.reshape(count * ways, row_width)
    empty = jnp.concatenate(
        [jnp.full((1, count), -jnp.inf, jnp.float32), jnp.zeros((7, count), jnp.float32)]
    )
    results = [jax.ShapeDtypeStruct((8, count), jnp.float32)]
    arranged = [
        jax.ShapeDtypeStruct((ways, count, width), jnp.bfloat16),
        jax.ShapeDtypeStruct((count, NOTES), jnp.bfloat16),
    ]
    near = chunks_of(core_index, held) + chunks_of(partner, crossed(held))
    body = functools.partial(first_body, len(near), share)
    outputs = results + arranged
    stats, tokens, notes = absorbed(body, (received, empty), near, count, outputs)
    body = functools.partial(next_body, len(far))
    for core, pieces in ((core_index, far), (partner, crossed(far))):
        (stats,) = absorbed(body, (tokens, notes, stats), chunks_of(core, pieces), count, results)

    stats = stats[:STATS].reshape(STATS, plane, share)
    sums = exchange(jnp.moveaxis(stats, 1, 0).reshape(plane, STATS * share), PLANE)
    part_peak = sums[:, :share]
    peak = jnp.max(part_peak, axis=0)
    rescale = jnp.exp(part_peak - peak[None])
    exp_sum = jnp.sum(sums[:, share : 2 * share] * rescale, axis=0)
    square_sum = jnp.sum(sums[:, 2 * share : 3 * share] * rescale * rescale, axis=0)
    label_logit = jnp.sum(sums[:, 3 * share :], axis=0)
    share_error = (
        square_sum / (exp_sum * exp_sum) - 2.0 * jnp.exp(label_logit - peak) / exp_sum + 1.0
    )
    token_error = to_everyone(share_error, "tensor").reshape(BLK_DEV, block_len)
    valid = jnp.arange(block_len, dtype=jnp.int32)[None, :] < local_lengths[:, None]
    return jnp.sum(jnp.where(valid, token_error, 0.0), axis=1) / local_lengths.astype(jnp.float32)


def solution(mesh):
    dp, tensor = mesh.shape["dp"], mesh.shape["tensor"]
    finer = Mesh(mesh.devices.reshape(*GRID, dp // (GRID[0] * GRID[1]), tensor), DP_TENSOR)
    placed = (P(DP, None, "tensor"), P(), P(DP_TENSOR, None), P(DP), P(DP), P(DP), P(DP, None))
    return jax.shard_map(per_device, mesh=finer, in_specs=placed, out_specs=P(DP), check_vma=False)
```
